32 devices in a mesh: dp: 2 (over x), fsdp: 16 (over z, y, core).
Axes of the slice: x: 2, y: 2, z: 4, core: 2. Of those that a mesh axis runs over, the one named last changes fastest.
Arguments:
- hidden: bfloat16 [2, 16384, 512], P(None, ('dp', 'fsdp')), parts along dimension 1
- targets: int32 [2, 16384], P(None, ('dp', 'fsdp')), parts along dimension 1
- w_out: bfloat16 [32128, 512], P('fsdp')
Outputs:
- output 1: float32 [4], P('dp'), parts along dimension 0
- output 2: float32 [2, 16384, 512], P(None, ('dp', 'fsdp')), parts along dimension 1
- output 3: float32 [64256, 512], P(('dp', 'fsdp')), parts along dimension 0
There are 2 independent parts. The reference program is written for one: setup_inputs(seed, part) draws one part's arguments, and reference() takes and returns one part's arrays. A program takes and returns all parts, laid end to end along the dimension named above; an argument that names none is the same for every part.
All inputs are finite; a program needn't handle non-finite values.
Results may differ from the reference program's by a relative error of at most 0.001.
Values are sent between devices in bfloat16 or wider.
A program may use at most 1 GiB of HBM per device.

```python
import jax
import jax.numpy as jnp
from jax import lax

TOK_DEV = 512
GROUP_SIZE = 16
VOCAB_SIZE = 32128
MODEL_DIM = 512

TOKENS_PART = TOK_DEV * GROUP_SIZE
VOCAB_BLK = VOCAB_SIZE // GROUP_SIZE


def setup_inputs(seed: int = 0, part: int = 0) -> dict:
    base_key = jax.random.key(seed)
    shared_key, parts_key = jax.random.split(base_key)
    part_key = jax.random.fold_in(parts_key, part)
    key_hid, key_tgt = jax.random.split(part_key)
    hidden = jax.random.normal(key_hid, (2, TOKENS_PART, MODEL_DIM), jnp.float32).astype(jnp.bfloat16)
    targets = jax.random.randint(key_tgt, (2, TOKENS_PART), 0, VOCAB_SIZE, jnp.int32)
    targets = targets.at[0, 0].set(0).at[1, TOKENS_PART - 1].set(VOCAB_SIZE - 1)
    w_scaled = jax.random.normal(shared_key, (VOCAB_SIZE, MODEL_DIM), jnp.float32) * MODEL_DIM ** -0.5
    return {'hidden': hidden, 'targets': targets, 'w_out': w_scaled.astype(jnp.bfloat16)}


def reference(hidden, targets, w_out):
    tok_blocks = hidden.reshape(2 * GROUP_SIZE, TOK_DEV, MODEL_DIM)
    tgt_blocks = targets.reshape(2 * GROUP_SIZE, TOK_DEV)
    w_blocks = w_out.reshape(GROUP_SIZE, VOCAB_BLK, MODEL_DIM)
    blk_ids = jnp.arange(GROUP_SIZE, dtype=jnp.int32)
    col_ids = jnp.arange(VOCAB_BLK, dtype=jnp.int32)[None, :]

    def block_logits(tok_rows, row_tgt, w_blk, blk_idx):
        logits = jnp.dot(tok_rows, w_blk.T, preferred_element_type=jnp.float32)
        tgt_hit = (row_tgt - blk_idx * VOCAB_BLK)[:, None] == col_ids
        return logits, tgt_hit

    def token_stats(blk_in):
        tok_rows, row_tgt = blk_in

        def vocab_step(run_stats, w_in):
            run_max, run_sum, tgt_logit = run_stats
            logits, tgt_hit = block_logits(tok_rows, row_tgt, w_in[0], w_in[1])
            tgt_logit = tgt_logit + jnp.sum(jnp.where(tgt_hit, logits, 0.0), axis=1)
            new_max = jnp.maximum(run_max, jnp.max(logits, axis=1))
            run_sum = run_sum * jnp.exp(run_max - new_max) + jnp.sum(jnp.exp(logits - new_max[:, None]), axis=1)
            return (new_max, run_sum, tgt_logit), None

        init_stats = (jnp.full((TOK_DEV,), -jnp.inf, jnp.float32), jnp.zeros((TOK_DEV,), jnp.float32), jnp.zeros((TOK_DEV,), jnp.float32))
        (run_max, run_sum, tgt_logit), _ = lax.scan(vocab_step, init_stats, (w_blocks, blk_ids))
        return run_max + jnp.log(run_sum), tgt_logit

    log_norm, tgt_logit = lax.map(token_stats, (tok_blocks, tgt_blocks))
    loss_vals = jnp.sum((log_norm - tgt_logit).reshape(2, TOKENS_PART), axis=1) / TOKENS_PART

    def token_grads(d_w, blk_in):
        tok_rows, row_tgt, row_norm = blk_in

        def vocab_step(d_rows, w_in):
            logits, tgt_hit = block_logits(tok_rows, row_tgt, w_in[0], w_in[1])
            soft_probs = jnp.exp(logits - row_norm[:, None])
            d_logits = ((soft_probs - tgt_hit.astype(jnp.float32)) / TOKENS_PART).astype(jnp.bfloat16)
            d_rows = d_rows + jnp.dot(d_logits, w_in[0], preferred_element_type=jnp.float32)
            d_w_blk = jnp.dot(d_logits.T, tok_rows, preferred_element_type=jnp.float32)
            return d_rows, d_w_blk

        d_rows, d_w_blocks = lax.scan(vocab_step, jnp.zeros((TOK_DEV, MODEL_DIM), jnp.float32), (w_blocks, blk_ids))
        return d_w + d_w_blocks.reshape(VOCAB_SIZE, MODEL_DIM), d_rows

    d_w, d_rows = lax.scan(token_grads, jnp.zeros((VOCAB_SIZE, MODEL_DIM), jnp.float32), (tok_blocks, tgt_blocks, log_norm))
    return loss_vals, d_rows.reshape(2, TOKENS_PART, MODEL_DIM), d_w
```

```python
import functools
import math

import jax
import jax.numpy as jnp
from jax import lax
from jax.experimental import pallas as pl
from jax.experimental.pallas import tpu as pltpu
from jax.sharding import PartitionSpec as P


LOG2E = math.log2(math.e)
LN2 = math.log(2.0)
TILE = 512
LANES = 128
NT = (((1,), (1,)), ((), ()))


def dot_nt(a, b):
    return lax.dot_general(a, b, NT, preferred_element_type=jnp.float32)


def stats_kernel(n_h, n_w, valid, *refs):
    h_refs, w_refs = refs[:n_h], refs[n_h:n_h + n_w]
    o_ref, m_ref, s_ref, z_ref = refs[n_h + n_w:]
    lane = lax.broadcasted_iota(jnp.int32, (1, LANES), 1)
    tiles = [(w, t) for w in range(n_w) for t in range(w_refs[0].shape[0] // TILE)]
    for h in range(n_h):
        def logits(i, h=h):
            w, t = tiles[i]
            z_ref[i % 2] = dot_nt(h_refs[h][...], w_refs[w][pl.ds(t * TILE, TILE), :])

        def fold(i):
            t = tiles[i][1]
            zs = []
            for k in range(TILE // LANES):
                z = z_ref[i % 2, :, k * LANES:(k + 1) * LANES]
                first = t * TILE + k * LANES
                if first + LANES > valid:
                    z = jnp.where(lane + first < valid, z, -jnp.inf)
                zs.append(z)
            new_max = functools.reduce(jnp.maximum, zs)
            if i > 0:
                old_max = m_ref[...]
                new_max = jnp.maximum(old_max, new_max)
            part = functools.reduce(jnp.add, [jnp.exp2((z - new_max) * LOG2E) for z in zs])
            if i > 0:
                part = s_ref[...] * jnp.exp2((old_max - new_max) * LOG2E) + part
            m_ref[...] = new_max
            s_ref[...] = part

        logits(0)
        for i in range(len(tiles)):
            if i + 1 < len(tiles):
                logits(i + 1)
            fold(i)
        m_lane = m_ref[...]
        m_row = jnp.max(m_lane, axis=1, keepdims=True)
        s_row = jnp.sum(s_ref[...] * jnp.exp2((m_lane - m_row) * LOG2E), axis=1, keepdims=True)
        lse = m_row + LN2 * jnp.log2(s_row)
        o_ref[pl.ds(h, 1), :] = jnp.broadcast_to(lse, (TILE, LANES)).T[0:1]


def stats_call(hs, ws, valid):
    n_h, n_w = len(hs), len(ws)
    return pl.pallas_call(
        functools.partial(stats_kernel, n_h, n_w, valid),
        out_shape=jax.ShapeDtypeStruct((n_h, TILE), jnp.float32),
        in_specs=[pl.BlockSpec(memory_space=pltpu.VMEM)] * (n_h + n_w),
        out_specs=pl.BlockSpec(memory_space=pltpu.VMEM),
        scratch_shapes=[pltpu.VMEM((TILE, LANES), jnp.float32), pltpu.VMEM((TILE, LANES), jnp.float32),
                        pltpu.VMEM((2, TILE, TILE), jnp.float32)],
        compiler_params=pltpu.CompilerParams(vmem_limit_bytes=48 * 2 ** 20),
        cost_estimate=pl.CostEstimate(flops=2 * n_h * n_w * TILE * 2048 * 512, bytes_accessed=10 ** 6, transcendentals=0),
    )(*hs, *ws)


def to_column(row):
    return jnp.broadcast_to(row, (LANES, TILE)).T


def dh_kernel(n_h, n_w, valid, base_ref, *refs):
    h_refs, w_refs = refs[:n_h], refs[n_h:n_h + n_w]
    aux_ref, o_ref, hit_ref, c_ref, y_ref, z_ref = refs[n_h + n_w:]
    lane = lax.broadcasted_iota(jnp.int32, (1, LANES), 1).astype(jnp.float32)
    tiles = [(w, t) for w in range(n_w) for t in range(w_refs[0].shape[0] // TILE)]
    for h in range(n_h):
        c_ref[...] = to_column(aux_ref[h, 0:1, :])
        y_ref[...] = to_column(aux_ref[h, 1:2, :])
        def logits(i, h=h):
            w, t = tiles[i]
            z_ref[i % 2] = dot_nt(h_refs[h][...], w_refs[w][pl.ds(t * TILE, TILE), :])

        def use(i, h=h):
            w, t = tiles[i]
            base = base_ref[w].astype(jnp.float32)
            grads = []
            hits = None
            for k in range(TILE // LANES):
                first = t * TILE + k * LANES
                z = z_ref[i % 2, :, k * LANES:(k + 1) * LANES]
                prob = jnp.exp2(z * LOG2E - c_ref[...])
                hit = y_ref[...] == lane + (base + first)
                grad = prob - jnp.where(hit, 2.0 ** -13, 0.0)
                if first + LANES > valid:
                    grad = jnp.where(lane + first < valid, grad, 0.0)
                grads.append(grad.astype(jnp.bfloat16))
                picked = jnp.where(hit, z, 0.0)
                hits = picked if hits is None else hits + picked
            part = jnp.dot(jnp.concatenate(grads, axis=1), w_refs[w][pl.ds(t * TILE, TILE), :],
                           preferred_element_type=jnp.float32)
            hits = jnp.sum(hits.reshape(TILE // 8, 8, LANES), axis=0)
            if i == 0:
                o_ref[h] = part
            else:
                o_ref[h] += part
            if i == 0 and h == 0:
                hit_ref[...] = hits
            else:
                hit_ref[...] += hits

        logits(0)
        for i in range(len(tiles)):
            if i + 1 < len(tiles):
                logits(i + 1)
            use(i)


def dh_call(base, hs, ws, aux, valid):
    n_h, n_w = len(hs), len(ws)
    return pl.pallas_call(
        functools.partial(dh_kernel, n_h, n_w, valid),
        out_shape=[jax.ShapeDtypeStruct((n_h, TILE, 512), jnp.float32), jax.ShapeDtypeStruct((8, LANES), jnp.float32)],
        in_specs=[pl.BlockSpec(memory_space=pltpu.SMEM)] + [pl.BlockSpec(memory_space=pltpu.VMEM)] * (n_h + n_w + 1),
        out_specs=[pl.BlockSpec(memory_space=pltpu.VMEM)] * 2,
        scratch_shapes=[pltpu.VMEM((TILE, LANES), jnp.float32), pltpu.VMEM((TILE, LANES), jnp.float32),
                        pltpu.VMEM((2, TILE, TILE), jnp.float32)],
        compiler_params=pltpu.CompilerParams(vmem_limit_bytes=48 * 2 ** 20),
        cost_estimate=pl.CostEstimate(flops=4 * n_h * n_w * TILE * 2048 * 512, bytes_accessed=10 ** 6, transcendentals=0),
    )(base, *hs, *ws, aux)


def dw_kernel(n_h, has_init, base_ref, w_ref, *refs):
    refs = list(refs)
    h_refs = [refs.pop(0) for _ in range(n_h)]
    aux_refs = [refs.pop(0) for _ in range(n_h)]
    init_ref = refs.pop(0) if has_init else None
    o_ref, acc_ref, z_ref = refs
    blk = pl.program_id(0)
    row = (lax.broadcasted_iota(jnp.int32, (TILE, LANES), 0) + (base_ref[0] + blk * TILE)).astype(jnp.float32)
    tiles = [(g, k) for g in range(n_h) for k in range(h_refs[0].shape[0])]
    acc_ref[...] = init_ref[...] if has_init else jnp.zeros_like(acc_ref)

    def logits(i):
        g, k = tiles[i]
        z_ref[i % 2] = dot_nt(w_ref[...], h_refs[g][k])

    def use(i):
        g, k = tiles[i]
        grads = []
        for l in range(TILE // LANES):
            cols = slice(l * LANES, (l + 1) * LANES)
            prob = jnp.exp2(z_ref[i % 2, :, cols] * LOG2E - aux_refs[g][k, 0:1, cols])
            hit = aux_refs[g][k, 1:2, cols] == row
            grads.append((prob - jnp.where(hit, 2.0 ** -13, 0.0)).astype(jnp.bfloat16))
        acc_ref[...] += jnp.dot(jnp.concatenate(grads, axis=1), h_refs[g][k], preferred_element_type=jnp.float32)

    logits(0)
    for i in range(len(tiles)):
        if i + 1 < len(tiles):
            logits(i + 1)
        use(i)
    o_ref[...] = acc_ref[...]


def dw_call(base, w, hs, auxs, init, valid):
    n_h = len(hs)
    full = lambda a: pl.BlockSpec(a.shape, lambda i: (0,) * a.ndim, pipeline_mode=pl.Buffered(1))
    rows = pl.BlockSpec((TILE, 512), lambda i: (i, 0))
    inits = [] if init is None else [init]
    return pl.pallas_call(
        functools.partial(dw_kernel, n_h, init is not None),
        grid=(2048 // TILE,),
        out_shape=jax.ShapeDtypeStruct((valid, 512), jnp.float32),
        in_specs=[pl.BlockSpec(memory_space=pltpu.SMEM), rows] + [full(a) for a in hs] + [full(a) for a in auxs] + [rows] * len(inits),
        out_specs=rows,
        scratch_shapes=[pltpu.VMEM((TILE, 512), jnp.float32), pltpu.VMEM((2, TILE, TILE), jnp.float32)],
        compiler_params=pltpu.CompilerParams(vmem_limit_bytes=48 * 2 ** 20),
        cost_estimate=pl.CostEstimate(flops=4 * n_h * 4 * TILE * 2048 * 512, bytes_accessed=10 ** 6, transcendentals=0),
    )(base, w, *hs, *auxs, *inits)


def solution(mesh):
    group = mesh.shape['fsdp']
    n_z = group // 4
    core_perm = [(i, i ^ 1) for i in range(group)]
    y_perm = [(i, i ^ 2) for i in range(group)]

    def send(x, perm):
        return lax.ppermute(x, 'fsdp', perm)

    def z_perm(k):
        return [(i, (i + 4 * k) % group) for i in range(group)]

    def local_head(hidden, targets, w_loc):
        rows = w_loc.shape[0]
        tokens = hidden.shape[1] * group
        me = lax.axis_index('fsdp')
        w0 = jnp.pad(w_loc, ((0, 2048 - rows), (0, 0)))
        w1 = send(w0, core_perm)
        w2 = send(w0, y_perm)
        w3 = send(w2, core_perm)
        ws = [w0, w1, w2, w3]
        bases = jnp.stack([me, me ^ 1, me ^ 2, me ^ 3]).astype(jnp.int32) * rows

        tgts = [targets] + [send(targets, z_perm(k)) for k in range(1, n_z)]
        pieces = []
        for m in range(2):
            ps = [hidden[m]]
            for k in range(1, n_z):
                ps.append(send(ps[-1], z_perm(1)))
            pieces.append(ps)

        aux, hit_sums, d_rows, lse_own = [], [], [], []
        for m in range(2):
            ps = pieces[m]
            parts = jnp.stack([stats_call(ps, ws[:2], rows), stats_call(ps, ws[2:], rows)])
            shifted = [parts] + [send(parts, z_perm(k)) for k in range(1, n_z)]
            allp = jnp.stack([jnp.stack([shifted[s][:, (k - s) % n_z] for s in range(n_z)]) for k in range(n_z)])
            allp = allp.reshape(n_z, 2 * n_z, TILE)
            top = jnp.max(allp, axis=1, keepdims=True)
            lse = top[:, 0] + jnp.log(jnp.sum(jnp.exp(allp - top), axis=1))
            lse_own.append(jnp.sum(lse[0]))
            ym = jnp.stack([t[m] for t in tgts]).astype(jnp.float32)
            aux.append(jnp.stack([lse * LOG2E + math.log2(tokens), ym], axis=1))

            p12, h12 = dh_call(bases, ps[1:3], ws, aux[m][1:3], rows)
            p30, h30 = dh_call(bases, [ps[3], ps[0]], ws, jnp.stack([aux[m][3], aux[m][0]]), rows)
            hit_sums.append(jnp.sum(h12) + jnp.sum(h30))
            acc = p12[0]
            acc = send(acc, z_perm(1)) + p12[1]
            acc = send(acc, z_perm(1)) + p30[0]
            d_rows.append(send(acc, z_perm(1)) + p30[1])

        g0 = [jnp.stack(ps) for ps in pieces]
        g1 = [send(g, core_perm) for g in g0]
        g2 = [send(g, y_perm) for g in g0]
        g3 = [send(g, core_perm) for g in g2]
        a1 = [send(a, core_perm) for a in aux]
        a2 = [send(a, y_perm) for a in aux]
        a3 = [send(a, core_perm) for a in a2]
        d_w = dw_call(bases, w0, g0 + g1, aux + a1, None, rows)
        d_w = dw_call(bases, w0, g2 + g3, a2 + a3, d_w, rows)

        part = jnp.stack(lse_own) - jnp.stack(hit_sums)
        for perm in (core_perm, y_perm, z_perm(1), z_perm(2)):
            part = part + send(part, perm)
        loss_vals = part / tokens
        return loss_vals, jnp.stack(d_rows), d_w

    return jax.shard_map(local_head, mesh=mesh,
                         in_specs=(P(None, ('dp', 'fsdp'), None), P(None, ('dp', 'fsdp')), P('fsdp', None)),
                         out_specs=(P('dp'), P(None, ('dp', 'fsdp'), None), P(('dp', 'fsdp'), None)),
                         check_vma=False)
```

```python
import functools
import math

import jax
import jax.numpy as jnp
from jax import lax
from jax.experimental import pallas as pl
from jax.experimental.pallas import tpu as pltpu
from jax.sharding import PartitionSpec as P

LOG2E = math.log2(math.e)
LN2 = math.log(2.0)
TILE = 512
LANES = 128
NQ = TILE // LANES
NZ = 4
MESH = pl.DeviceIdType.MESH
NT = (((1,), (1,)), ((), ()))
F32 = jnp.float32


def dot_nt(a, b):
    return lax.dot_general(a, b, NT, preferred_element_type=F32)


def to_column(row):
    return jnp.broadcast_to(row, (LANES, TILE)).T


COUNTS = dict(W1=1, W2=4, W3=4, H=6, Y=3, L=6, A1=2, A2=2, A3=2, G1=2, G2=2, G3=2, R=6, S=5)
FIRST = {}
for _name, _n in COUNTS.items():
    FIRST[_name] = sum(COUNTS[k] for k in FIRST)
N_SEM = sum(COUNTS.values())


def head_kernel(group, valid, tokens, h_hbm, w_hbm, y_ref, loss_o, dh_o, dw_hbm,
                hb, wb, yb, lp, lr, ab, rs, dh, acc, m_st, s_st, z_ref, c_col, y_col, hits, vb, vr,
                send_sem, recv_sem, load_sem):
    me = lax.axis_index('fsdp')
    core = me + 1 - 2 * lax.rem(me, 2)
    yid = lax.rem(me // 2, 2)
    ypeer = me + 2 - 4 * yid
    zpeer = [lax.rem(me + 4 * s, group) for s in range(NZ)]
    lane = lax.broadcasted_iota(jnp.int32, (1, LANES), 1)
    lane_f = lane.astype(F32)

    def copy(name, j, src, dst, to):
        i = FIRST[name] + j
        return pltpu.make_async_remote_copy(src_ref=src, dst_ref=dst, send_sem=send_sem.at[i], recv_sem=recv_sem.at[i],
                                            device_id={'fsdp': to}, device_id_type=MESH)

    def rows(i):
        return pl.ds(i * TILE, TILE)

    w1 = copy('W1', 0, wb.at[0], wb.at[1], core)
    w2 = [copy('W2', i, wb.at[0, rows(i)], wb.at[2, rows(i)], ypeer) for i in range(4)]
    w3 = [copy('W3', i, wb.at[2, rows(i)], wb.at[3, rows(i)], core) for i in range(4)]
    hs = [[None] + [copy('H', 3 * m + k - 1, hb.at[0, m, k - 1], hb.at[0, m, k], zpeer[1]) for k in range(1, NZ)] for m in range(2)]
    ys = [copy('Y', k - 1, y_ref, yb.at[k - 1], zpeer[k]) for k in range(1, NZ)]
    ls = [[copy('L', 3 * m + s - 1, lp.at[m], lr.at[m, s - 1], zpeer[s]) for s in range(1, NZ)] for m in range(2)]
    a1 = [copy('A1', m, ab.at[0, m], ab.at[1, m], core) for m in range(2)]
    a2 = [copy('A2', m, ab.at[0, m], ab.at[2, m], ypeer) for m in range(2)]
    a3 = [copy('A3', m, ab.at[2, m], ab.at[3, m], core) for m in range(2)]
    g1 = [copy('G1', m, hb.at[0, m], hb.at[1, m], core) for m in range(2)]
    g2 = [copy('G2', m, hb.at[0, m], hb.at[2, m], ypeer) for m in range(2)]
    g3 = [copy('G3', m, hb.at[2, m], hb.at[3, m], core) for m in range(2)]
    rr = [[copy('R', 3 * m + j, dh.at[m, j + 1], rs.at[m, j], zpeer[1]) for j in range(3)] for m in range(2)]
    ss = [copy('S', s - 1, vb.at[0], vr.at[s - 1], zpeer[s]) for s in range(1, NZ)]
    ss.append(copy('S', 3, vb.at[1], vr.at[3], core))
    ss.append(copy('S', 4, vb.at[2], vr.at[4], ypeer))
    every = [w1] + w2 + w3 + hs[0][1:] + hs[1][1:] + ys + ls[0] + ls[1] + a1 + a2 + a3 + g1 + g2 + g3 + rr[0] + rr[1] + ss

    loads = [pltpu.make_async_copy(h_hbm.at[m], hb.at[0, m, 0], load_sem.at[m]) for m in range(2)]
    load_w = pltpu.make_async_copy(w_hbm, wb.at[0], load_sem.at[2])
    loads[0].start()
    load_w.start()
    loads[1].start()

    barrier = pltpu.get_barrier_semaphore()
    for peer in (core, ypeer, zpeer[1], zpeer[2], zpeer[3]):
        pl.semaphore_signal(barrier, inc=1, device_id={'fsdp': peer}, device_id_type=MESH)
    m_st[...] = jnp.full(m_st.shape, -jnp.inf, F32)
    s_st[...] = jnp.zeros(s_st.shape, F32)
    lp[...] = jnp.zeros(lp.shape, F32)
    pl.semaphore_wait(barrier, 5)
    loads[0].wait()
    hs[0][1].start()
    load_w.wait()
    for c in w2:
        c.start()
    w1.start()
    for c in ys:
        c.start()
    loads[1].wait()

    def run_stats(n, unit):
        def logits(u, t, slot):
            m, k, p, half = unit(u)
            start = pl.multiple_of((2 * half + t % 2) * TILE, TILE)
            z_ref[slot] = dot_nt(hb[0, m, k], wb[2 * p + t // 2, pl.ds(start, TILE), :])

        def fold(u, t, slot):
            m, k, p, half = unit(u)
            first = (2 * half + t % 2) * TILE
            zs = [z_ref[slot, :, q * LANES:(q + 1) * LANES] for q in range(NQ)]
            if t % 2 == 1:
                zs[-1] = jnp.where(lane + (first + TILE - LANES) < valid, zs[-1], -jnp.inf)
            old_max = m_st[m, k]
            new_max = jnp.maximum(old_max, functools.reduce(jnp.maximum, zs))
            part = functools.reduce(jnp.add, [jnp.exp2((z - new_max) * LOG2E) for z in zs])
            s_st[m, k] = s_st[m, k] * jnp.exp2((old_max - new_max) * LOG2E) + part
            m_st[m, k] = new_max

        logits(0, 0, 0)

        def body(u, carry):
            for t in range(4):
                if t < 3:
                    logits(u, t + 1, (t + 1) % 2)
                else:
                    logits(jnp.minimum(u + 1, n - 1), 0, 0)
                fold(u, t, t % 2)
            return carry
        lax.fori_loop(0, n, body, 0)

    def finalize(m):
        for k in range(NZ):
            m_lane = m_st[m, k]
            m_row = jnp.max(m_lane, axis=1, keepdims=True)
            s_row = jnp.sum(s_st[m, k] * jnp.exp2((m_lane - m_row) * LOG2E), axis=1, keepdims=True)
            lse = m_row + LN2 * jnp.log2(s_row)
            lp[m, k:k + 1, :] = jnp.broadcast_to(lse, (TILE, LANES)).T[0:1]

    def combine(m):
        for k in range(NZ):
            parts = [lp[m, k:k + 1, :]]
            for s in range(1, NZ):
                j = (k - s) % NZ
                parts.append(lr[m, s - 1, j:j + 1, :])
            top = functools.reduce(jnp.maximum, parts)
            total = functools.reduce(jnp.add, [jnp.exp2((x - top) * LOG2E) for x in parts])
            lse = top + LN2 * jnp.log2(total)
            ab[0, m, k:k + 1, :] = lse * LOG2E + math.log2(tokens)
            tgt = y_ref if k == 0 else yb.at[k - 1]
            ab[0, m, NZ + k:NZ + k + 1, :] = tgt[m:m + 1, :]
            if k == 0:
                own = functools.reduce(jnp.add, [lse[:, q * LANES:(q + 1) * LANES] for q in range(NQ)])
                hits[m] = jnp.zeros((8, LANES), F32)
                vb[0, 8 * m:8 * m + 8, :] = jnp.zeros((8, LANES), F32)
                vb[0, 8 * m:8 * m + 1, :] = own

    def share(m):
        for c in (a1[m], a2[m], g1[m], g2[m]):
            c.start()

    w1.wait_recv()
    run_stats(4, lambda u: (u // 2, 0, 0, lax.rem(u, 2)))
    hs[0][1].wait_recv()
    hs[0][2].start()
    run_stats(2, lambda u: (0, 1, 0, u))
    w2[0].wait_recv()
    w3[0].start()
    w2[1].wait_recv()
    w3[1].start()
    hs[0][2].wait_recv()
    hs[0][3].start()
    run_stats(2, lambda u: (0, 2, 0, u))
    w3[0].wait_recv()
    w3[1].wait_recv()
    run_stats(3, lambda u: (0, u, 1, 0))
    w2[2].wait_recv()
    w3[2].start()
    hs[0][3].wait_recv()
    hs[1][1].start()
    run_stats(3, lambda u: (0, 3, u // 2, lax.rem(u, 2)))
    w2[3].wait_recv()
    w3[3].start()
    w3[2].wait_recv()
    w3[3].wait_recv()
    run_stats(4, lambda u: (0, u, 1, 1))
    finalize(0)
    for c in ls[0]:
        c.start()
    run_stats(2, lambda u: (1, 0, 1, u))
    hs[1][1].wait_recv()
    hs[1][2].start()
    for c in ys:
        c.wait_recv()
    for c in ls[0]:
        c.wait_recv()
    combine(0)
    share(0)

    base = [(me + (1 - 2 * lax.rem(me, 2)) * (w % 2) + (2 - 4 * yid) * (w // 2)) * valid for w in range(4)]

    def dh_step(i, carry):
        m = i // 4
        k = lax.rem(i + 1, NZ)
        c_col[...] = to_column(ab[0, m, pl.ds(k, 1), :])
        y_col[...] = to_column(ab[0, m, pl.ds(k + NZ, 1), :])
        tiles = [(w, t) for w in range(4) for t in range(4)]

        def logits(j):
            w, t = tiles[j]
            z_ref[j % 2] = dot_nt(hb[0, m, k], wb[w, rows(t), :])

        logits(0)
        for j, (w, t) in enumerate(tiles):
            if j + 1 < len(tiles):
                logits(j + 1)
            grads = []
            found = None
            for q in range(NQ):
                first = t * TILE + q * LANES
                z = z_ref[j % 2, :, q * LANES:(q + 1) * LANES]
                prob = jnp.exp2(z * LOG2E - c_col[...])
                hit = y_col[...] == lane_f + (base[w] + first).astype(F32)
                grad = prob - jnp.where(hit, 1.0 / tokens, 0.0)
                if first + LANES > valid:
                    grad = jnp.where(lane + first < valid, grad, 0.0)
                grads.append(grad.astype(jnp.bfloat16))
                picked = jnp.where(hit, z, 0.0)
                found = picked if found is None else found + picked
            part = jnp.dot(jnp.concatenate(grads, axis=1), wb[w, rows(t), :], preferred_element_type=F32)
            if j == 0:
                dh[m, k] = part
            else:
                dh[m, k] += part
            hits[m] += jnp.sum(found.reshape(TILE // 8, 8, LANES), axis=0)

        @pl.when(i == 0)
        def _():
            rr[0][0].start()
            hs[1][2].wait_recv()
            hs[1][3].start()

        @pl.when(i == 1)
        def _():
            run_stats(8, lambda u: (1, 1 + u // 4, lax.rem(u, 4) // 2, lax.rem(u, 2)))
            hs[1][3].wait_recv()
            run_stats(4, lambda u: (1, 3, u // 2, lax.rem(u, 2)))
            finalize(1)
            for c in ls[1]:
                c.start()
            rr[0][0].wait_recv()
            dh[0, 2] += rs[0, 0]
            rr[0][1].start()

        @pl.when(i == 2)
        def _():
            for c in ls[1]:
                c.wait_recv()
            combine(1)
            share(1)

        @pl.when(i == 3)
        def _():
            for c in (g2[0], a2[0]):
                c.wait_recv()
            g3[0].start()
            a3[0].start()

        @pl.when(i == 4)
        def _():
            rr[0][1].wait_recv()
            dh[0, 3] += rs[0, 1]
            rr[0][2].start()
            rr[1][0].start()
        return carry

    lax.fori_loop(0, 8, dh_step, 0)

    for m in range(2):
        vb[0, 8 * m:8 * m + 8, :] = vb[0, 8 * m:8 * m + 8, :] - hits[m]
    rr[0][2].wait_recv()
    dh_o[0] = dh[0, 0] + rs[0, 2]
    for c in ss[:3]:
        c.start()
    for c in (g2[1], a2[1]):
        c.wait_recv()
    g3[1].start()
    a3[1].start()
    for c in g1 + a1:
        c.wait_recv()

    acc[...] = jnp.zeros(acc.shape, F32)
    base0 = me * valid
    outs = [pltpu.make_async_copy(acc.at[pl.ds(r * TILE, min(TILE, valid - r * TILE))],
                                  dw_hbm.at[pl.ds(r * TILE, min(TILE, valid - r * TILE))], load_sem.at[3 + r]) for r in range(4)]

    def dw_step(i, carry):
        g = i // 4
        r = lax.rem(i, 4)
        start = pl.multiple_of(r * TILE, TILE)
        row = (lax.broadcasted_iota(jnp.int32, (TILE, LANES), 0) + (base0 + r * TILE)).astype(F32)
        tiles = [(m, k) for m in range(2) for k in range(NZ)]

        def logits(j):
            m, k = tiles[j]
            z_ref[j % 2] = dot_nt(wb[0, pl.ds(start, TILE), :], hb[g, m, k])

        logits(0)
        for j, (m, k) in enumerate(tiles):
            if j + 1 < len(tiles):
                logits(j + 1)
            grads = []
            for q in range(NQ):
                cols = slice(q * LANES, (q + 1) * LANES)
                prob = jnp.exp2(z_ref[j % 2, :, cols] * LOG2E - ab[g, m, k:k + 1, cols])
                hit = ab[g, m, NZ + k:NZ + k + 1, cols] == row
                grads.append((prob - jnp.where(hit, 1.0 / tokens, 0.0)).astype(jnp.bfloat16))
            acc[pl.ds(start, TILE), :] += jnp.dot(jnp.concatenate(grads, axis=1), hb[g, m, k], preferred_element_type=F32)

        @pl.when(i == 3)
        def _():
            for c in ss[:3]:
                c.wait_recv()
            vb[1] = vb[0] + vr[0] + vr[1] + vr[2]
            ss[3].start()
            rr[1][0].wait_recv()
            dh[1, 2] += rs[1, 0]
            rr[1][1].start()

        @pl.when(i == 7)
        def _():
            ss[3].wait_recv()
            vb[2] = vb[1] + vr[3]
            ss[4].start()
            for c in g3 + a3:
                c.wait_recv()

        @pl.when(i == 9)
        def _():
            rr[1][1].wait_recv()
            dh[1, 3] += rs[1, 1]
            rr[1][2].start()

        for rr_i in range(4):
            @pl.when(i == 12 + rr_i)
            def _():
                outs[rr_i].start()
        return carry

    lax.fori_loop(0, 16, dw_step, 0)
    ss[4].wait_recv()
    loss_o[...] = vb[2] + vr[4]
    rr[1][2].wait_recv()
    dh_o[1] = dh[1, 0] + rs[1, 2]
    for c in outs:
        c.wait()
    for c in every:
        c.wait_send()


def solution(mesh):
    group = mesh.shape['fsdp']

    def local_head(hidden, targets, w_loc):
        valid = w_loc.shape[0]
        tokens = hidden.shape[1] * group
        bf = jnp.bfloat16
        w0 = jnp.pad(w_loc, ((0, 2048 - valid), (0, 0)))
        y = jnp.pad(targets.astype(F32), ((0, 6), (0, 0)))
        any_spec = pl.BlockSpec(memory_space=pl.ANY)
        vmem = pl.BlockSpec(memory_space=pltpu.VMEM)
        loss, d_h, d_w = pl.pallas_call(
            functools.partial(head_kernel, group, valid, tokens),
            out_shape=[jax.ShapeDtypeStruct((16, LANES), F32), jax.ShapeDtypeStruct((2, TILE, 512), F32),
                       jax.ShapeDtypeStruct((valid, 512), F32)],
            in_specs=[any_spec, any_spec, vmem],
            out_specs=[vmem, vmem, any_spec],
            scratch_shapes=[
                pltpu.VMEM((4, 2, NZ, TILE, 512), bf),
                pltpu.VMEM((4, 2048, 512), bf),
                pltpu.VMEM((3, 8, TILE), F32),
                pltpu.VMEM((2, 8, TILE), F32),
                pltpu.VMEM((2, 3, 8, TILE), F32),
                pltpu.VMEM((4, 2, 8, TILE), F32),
                pltpu.VMEM((2, 3, TILE, 512), F32),
                pltpu.VMEM((2, NZ, TILE, 512), F32),
                pltpu.VMEM((2048, 512), F32),
                pltpu.VMEM((2, NZ, TILE, LANES), F32),
                pltpu.VMEM((2, NZ, TILE, LANES), F32),
                pltpu.VMEM((2, TILE, TILE), F32),
                pltpu.VMEM((TILE, LANES), F32),
                pltpu.VMEM((TILE, LANES), F32),
                pltpu.VMEM((2, 8, LANES), F32),
                pltpu.VMEM((3, 16, LANES), F32),
                pltpu.VMEM((5, 16, LANES), F32),
                pltpu.SemaphoreType.DMA((N_SEM,)),
                pltpu.SemaphoreType.DMA((N_SEM,)),
                pltpu.SemaphoreType.DMA((7,)),
            ],
            compiler_params=pltpu.CompilerParams(collective_id=0, has_side_effects=True, vmem_limit_bytes=67043328),
        )(hidden, w0, y)
        loss_vals = jnp.sum(loss.reshape(2, 8 * LANES), axis=1) / tokens
        return loss_vals, d_h, d_w

    return jax.shard_map(local_head, mesh=mesh,
                         in_specs=(P(None, ('dp', 'fsdp'), None), P(None, ('dp', 'fsdp')), P('fsdp', None)),
                         out_specs=(P('dp'), P(None, ('dp', 'fsdp'), None), P(('dp', 'fsdp'), None)),
                         check_vma=False)
```

```python
import functools
import math

import jax
import jax.numpy as jnp
from jax import lax
from jax.experimental import pallas as pl
from jax.experimental.pallas import tpu as pltpu
from jax.sharding import PartitionSpec as P

LOG2E = math.log2(math.e)
LN2 = math.log(2.0)
TILE = 512
LANES = 128
NQ = TILE // LANES
NZ = 4
MESH = pl.DeviceIdType.MESH
NT = (((1,), (1,)), ((), ()))
TN = (((0,), (0,)), ((), ()))
F32 = jnp.float32


def dot_nt(a, b):
    return lax.dot_general(a, b, NT, preferred_element_type=F32)


def to_column(row):
    return jnp.broadcast_to(row, (LANES, TILE)).T


COUNTS = dict(W1=1, W2=2, WX=2, W3=4, H=12, Y=3, L=6, A2=2, A3=2, G2=2, G3=2, R=12, S=5, D=1)
FIRST = {}
for _name, _n in COUNTS.items():
    FIRST[_name] = sum(COUNTS[k] for k in FIRST)
N_SEM = sum(COUNTS.values())


def head_kernel(group, valid, tokens, h_hbm, w_hbm, y_in, loss_o, dh_o, dw_hbm,
                hb, wb, yb, lp, lr, ab, rs, dh, dwa, dwr, m_st, s_st, z_ref, c_col, y_col, hits, vb, vr,
                send_sem, recv_sem, load_sem):
    me = lax.axis_index('fsdp')
    xid = lax.axis_index('dp')
    core = me + 1 - 2 * lax.rem(me, 2)
    yid = lax.rem(me // 2, 2)
    ypeer = me + 2 - 4 * yid
    zpeer = [lax.rem(me + 4 * s, group) for s in range(NZ)]
    lane = lax.broadcasted_iota(jnp.int32, (1, LANES), 1)
    lane_f = lane.astype(F32)

    def copy(name, j, src, dst, to, axis='fsdp'):
        i = FIRST[name] + j
        return pltpu.make_async_remote_copy(src_ref=src, dst_ref=dst, send_sem=send_sem.at[i], recv_sem=recv_sem.at[i],
                                            device_id={axis: to}, device_id_type=MESH)

    def rows(i):
        return pl.ds(i * TILE, TILE)

    def wrows(half, i):
        return pl.ds(pl.multiple_of((2 * half + i) * TILE, TILE), TILE)

    def halves(i):
        return pl.ds(i * (TILE // 2), TILE // 2)

    xpeer = 1 - xid
    w1 = copy('W1', 0, wb.at[0], wb.at[1], core)
    w2 = [copy('W2', i, wb.at[0, wrows(xid, i)], wb.at[2, wrows(xid, i)], ypeer) for i in range(2)]
    wx = [copy('WX', i, wb.at[2, wrows(xid, i)], wb.at[2, wrows(xid, i)], xpeer, 'dp') for i in range(2)]
    w3 = [copy('W3', 2 * e + i, wb.at[2, wrows(half, i)], wb.at[3, wrows(half, i)], core)
          for e, half in enumerate((xid, xpeer)) for i in range(2)]
    hs = [[None] + [[copy('H', 6 * m + 2 * (k - 1) + i, hb.at[0, m, k - 1, halves(i)], hb.at[0, m, k, halves(i)], zpeer[1])
                     for i in range(2)] for k in range(1, NZ)] for m in range(2)]
    ys = [copy('Y', k - 1, yb.at[0], yb.at[k], zpeer[k]) for k in range(1, NZ)]
    ls = [[copy('L', 3 * m + j - 1, lp.at[m], lr.at[m, j - 1], zpeer[j]) for j in range(1, NZ)] for m in range(2)]
    a2 = [copy('A2', m, ab.at[0, m], ab.at[1, m], ypeer) for m in range(2)]
    a3 = [copy('A3', m, ab.at[1, m], ab.at[2, m], core) for m in range(2)]
    g2 = [copy('G2', m, hb.at[0, m], hb.at[1, m], ypeer) for m in range(2)]
    g3 = [copy('G3', m, hb.at[1, m], hb.at[2, m], core) for m in range(2)]
    rr = [[[copy('R', 6 * m + 2 * j + i, dh.at[m, j + 1, halves(i)], rs.at[m, j, halves(i)], zpeer[1]) for i in range(2)]
           for j in range(3)] for m in range(2)]
    ss = [copy('S', j - 1, vb.at[0], vr.at[j - 1], zpeer[j]) for j in range(1, NZ)]
    ss.append(copy('S', 3, vb.at[1], vr.at[3], core))
    ss.append(copy('S', 4, vb.at[2], vr.at[4], ypeer))
    dw_copy = copy('D', 0, dwa.at[1], dwr, core)
    every = [w1, dw_copy] + w2 + wx + w3 + ys + ls[0] + ls[1] + a2 + a3 + g2 + g3 + ss
    for m in range(2):
        every += [c for pair in hs[m][1:] + rr[m] for c in pair]

    def pass_on(m, k, i):
        hs[m][k][i].wait_recv()
        if k + 1 < NZ:
            hs[m][k + 1][i].start()

    def hop(m, j, i):
        if j > 0:
            rr[m][j - 1][i].wait_recv()
            dh[m, j + 1, halves(i), :] += rs[m, j - 1, halves(i), :]
        rr[m][j][i].start()

    loads = [pltpu.make_async_copy(h_hbm.at[m], hb.at[0, m, 0], load_sem.at[m]) for m in range(2)]
    loads[0].start()
    loads[1].start()
    clear = (valid // 16) * 16
    wb[0, clear:, :] = jnp.zeros((2048 - clear, 512), jnp.bfloat16)
    load_w = pltpu.make_async_copy(w_hbm, wb.at[0, pl.ds(0, valid)], load_sem.at[2])
    load_w.start()

    barrier = pltpu.get_barrier_semaphore()
    for peer in (core, ypeer, zpeer[1], zpeer[2], zpeer[3]):
        pl.semaphore_signal(barrier, inc=1, device_id={'fsdp': peer}, device_id_type=MESH)
    pl.semaphore_signal(barrier, inc=1, device_id={'dp': xpeer}, device_id_type=MESH)
    yb[0] = jnp.concatenate([y_in[...].astype(F32), jnp.zeros((6, TILE), F32)], axis=0)
    m_st[...] = jnp.full(m_st.shape, -jnp.inf, F32)
    s_st[...] = jnp.zeros(s_st.shape, F32)
    lp[...] = jnp.zeros(lp.shape, F32)
    pl.semaphore_wait(barrier, 6)
    loads[0].wait()
    for i in range(2):
        hs[0][1][i].start()
    load_w.wait()
    for c in w2:
        c.start()
    w1.start()
    for c in ys:
        c.start()
    loads[1].wait()

    def run_stats(n, unit):
        def logits(u, t, slot):
            m, k, p, half = unit(u)
            start = pl.multiple_of((2 * half + t % 2) * TILE, TILE)
            z_ref[slot] = dot_nt(hb[0, m, k], wb[2 * p + t // 2, pl.ds(start, TILE), :])

        def fold(u, t, slot):
            m, k, p, half = unit(u)
            first = (2 * half + t % 2) * TILE
            zs = [z_ref[slot, :, q * LANES:(q + 1) * LANES] for q in range(NQ)]
            if t % 2 == 1:
                zs[-1] = jnp.where(lane + (first + TILE - LANES) < valid, zs[-1], -jnp.inf)
            old_max = m_st[m, k]
            new_max = jnp.maximum(old_max, functools.reduce(jnp.maximum, zs))
            part = functools.reduce(jnp.add, [jnp.exp2((z - new_max) * LOG2E) for z in zs])
            s_st[m, k] = s_st[m, k] * jnp.exp2((old_max - new_max) * LOG2E) + part
            m_st[m, k] = new_max

        logits(0, 0, 0)

        def body(u, carry):
            for t in range(4):
                if t < 3:
                    logits(u, t + 1, (t + 1) % 2)
                else:
                    logits(jnp.minimum(u + 1, n - 1), 0, 0)
                fold(u, t, t % 2)
            return carry
        lax.fori_loop(0, n, body, 0)

    def finalize(m):
        for k in range(NZ):
            m_lane = m_st[m, k]
            m_row = jnp.max(m_lane, axis=1, keepdims=True)
            s_row = jnp.sum(s_st[m, k] * jnp.exp2((m_lane - m_row) * LOG2E), axis=1, keepdims=True)
            lse = m_row + LN2 * jnp.log2(s_row)
            lp[m, k:k + 1, :] = jnp.broadcast_to(lse, (TILE, LANES)).T[0:1]

    def combine(m):
        for k in range(NZ):
            parts = [lp[m, k:k + 1, :]]
            for s in range(1, NZ):
                j = (k - s) % NZ
                parts.append(lr[m, s - 1, j:j + 1, :])
            top = functools.reduce(jnp.maximum, parts)
            total = functools.reduce(jnp.add, [jnp.exp2((x - top) * LOG2E) for x in parts])
            lse = top + LN2 * jnp.log2(total)
            ab[0, m, k:k + 1, :] = lse * LOG2E + math.log2(tokens)
            ab[0, m, NZ + k:NZ + k + 1, :] = yb[k, m:m + 1, :]
            if k == 0:
                own = functools.reduce(jnp.add, [lse[:, q * LANES:(q + 1) * LANES] for q in range(NQ)])
                hits[m] = jnp.zeros((8, LANES), F32)
                vb[0, 8 * m:8 * m + 8, :] = jnp.zeros((8, LANES), F32)
                vb[0, 8 * m:8 * m + 1, :] = own

    w1.wait_recv()
    run_stats(4, lambda u: (u // 2, 0, 0, lax.rem(u, 2)))
    pass_on(0, 1, 0)
    pass_on(0, 1, 1)
    w2[0].wait_recv()
    wx[0].start()
    w3[0].start()
    run_stats(2, lambda u: (0, 1, 0, u))
    pass_on(0, 2, 0)
    w2[1].wait_recv()
    wx[1].start()
    w3[1].start()
    pass_on(0, 2, 1)
    run_stats(2, lambda u: (0, 2, 0, u))
    wx[0].wait_recv()
    w3[2].start()
    w3[0].wait_recv()
    w3[1].wait_recv()
    run_stats(3, lambda u: (0, u, 1, xid))
    for i in range(2):
        pass_on(0, 3, i)
        hs[1][1][i].start()
    g2[0].start()
    run_stats(3, lambda u: (0, 3, u // 2, jnp.where(u == 2, xid, lax.rem(u, 2))))
    wx[1].wait_recv()
    w3[3].start()
    w3[2].wait_recv()
    w3[3].wait_recv()
    run_stats(4, lambda u: (0, u, 1, xpeer))
    finalize(0)
    for c in ls[0]:
        c.start()
    pass_on(1, 1, 0)
    run_stats(2, lambda u: (1, 0, 1, u))
    pass_on(1, 1, 1)
    for c in ys:
        c.wait_recv()
    for c in ls[0]:
        c.wait_recv()
    combine(0)
    a2[0].start()
    dwa[...] = jnp.zeros(dwa.shape, F32)

    base = [(me + (1 - 2 * lax.rem(me, 2)) * (w % 2) + (2 - 4 * yid) * (w // 2)) * valid for w in range(4)]

    def dh_step(i, carry):
        m = i // 4
        k = lax.rem(i + 1, NZ)
        c_col[...] = to_column(ab[0, m, pl.ds(k, 1), :])
        y_col[...] = to_column(ab[0, m, pl.ds(k + NZ, 1), :])
        tiles = [(w, t) for w in range(4) for t in range(4)]

        def logits(j):
            w, t = tiles[j]
            z_ref[j % 2] = dot_nt(hb[0, m, k], wb[w, rows(t), :])

        logits(0)
        for j, (w, t) in enumerate(tiles):
            if j + 1 < len(tiles):
                logits(j + 1)
            grads = []
            found = None
            for q in range(NQ):
                first = t * TILE + q * LANES
                z = z_ref[j % 2, :, q * LANES:(q + 1) * LANES]
                prob = jnp.exp2(z * LOG2E - c_col[...])
                hit = y_col[...] == lane_f + (base[w] + first).astype(F32)
                grad = prob - jnp.where(hit, 1.0 / tokens, 0.0)
                if first + LANES > valid:
                    grad = jnp.where(lane + first < valid, grad, 0.0)
                grads.append(grad.astype(jnp.bfloat16))
                picked = jnp.where(hit, z, 0.0)
                found = picked if found is None else found + picked
            grad_tile = jnp.concatenate(grads, axis=1)
            part = jnp.dot(grad_tile, wb[w, rows(t), :], preferred_element_type=F32)
            if j == 0:
                dh[m, k] = part
            else:
                dh[m, k] += part
            if w < 2:
                dwa[w, rows(t), :] += lax.dot_general(grad_tile, hb[0, m, k], TN, preferred_element_type=F32)
            hits[m] += jnp.sum(found.reshape(TILE // 8, 8, LANES), axis=0)

        @pl.when(i == 0)
        def _():
            pass_on(1, 2, 0)
            pass_on(1, 2, 1)
            hop(0, 0, 0)
            hop(0, 0, 1)

        @pl.when(i == 1)
        def _():
            run_stats(8, lambda u: (1, 1 + u // 4, lax.rem(u, 4) // 2, lax.rem(u, 2)))
            pass_on(1, 3, 0)
            pass_on(1, 3, 1)
            g2[1].start()
            run_stats(4, lambda u: (1, 3, u // 2, lax.rem(u, 2)))
            finalize(1)
            for c in ls[1]:
                c.start()
            hop(0, 1, 0)

        @pl.when(i == 2)
        def _():
            hop(0, 1, 1)
            for c in ls[1]:
                c.wait_recv()
            combine(1)
            a2[1].start()
            for c in (g2[0], a2[0]):
                c.wait_recv()
            g3[0].start()
            a3[0].start()

        @pl.when(i == 3)
        def _():
            hop(0, 2, 0)

        @pl.when(i == 4)
        def _():
            hop(0, 2, 1)
            hop(1, 0, 0)
            hop(1, 0, 1)

        @pl.when(i == 6)
        def _():
            for c in rr[0][2]:
                c.wait_recv()
            dh_o[0] = dh[0, 0] + rs[0, 2]
            for c in (g2[1], a2[1]):
                c.wait_recv()
            g3[1].start()
            a3[1].start()

        return carry

    lax.fori_loop(0, 8, dh_step, 0)

    for m in range(2):
        vb[0, 8 * m:8 * m + 8, :] = vb[0, 8 * m:8 * m + 8, :] - hits[m]
    for c in ss[:3]:
        c.start()
    hop(1, 1, 0)
    dw_copy.start()

    base0 = me * valid
    outs = [pltpu.make_async_copy(dwa.at[0, pl.ds(r * TILE, min(TILE, valid - r * TILE))],
                                  dw_hbm.at[pl.ds(r * TILE, min(TILE, valid - r * TILE))], load_sem.at[3 + r]) for r in range(4)]

    def dw_step(i, carry):
        g = 1 + i // 4
        r = lax.rem(i, 4)
        start = pl.multiple_of(r * TILE, TILE)
        row = (lax.broadcasted_iota(jnp.int32, (TILE, LANES), 0) + (base0 + r * TILE)).astype(F32)
        tiles = [(m, k) for m in range(2) for k in range(NZ)]

        def logits(j):
            m, k = tiles[j]
            z_ref[j % 2] = dot_nt(wb[0, pl.ds(start, TILE), :], hb[g, m, k])

        logits(0)
        for j, (m, k) in enumerate(tiles):
            if j + 1 < len(tiles):
                logits(j + 1)
            grads = []
            for q in range(NQ):
                cols = slice(q * LANES, (q + 1) * LANES)
                prob = jnp.exp2(z_ref[j % 2, :, cols] * LOG2E - ab[g, m, k:k + 1, cols])
                hit = ab[g, m, NZ + k:NZ + k + 1, cols] == row
                grads.append((prob - jnp.where(hit, 1.0 / tokens, 0.0)).astype(jnp.bfloat16))
            dwa[0, pl.ds(start, TILE), :] += jnp.dot(jnp.concatenate(grads, axis=1), hb[g, m, k], preferred_element_type=F32)

        @pl.when(i == 1)
        def _():
            for c in ss[:3]:
                c.wait_recv()
            vb[1] = vb[0] + vr[0] + vr[1] + vr[2]
            ss[3].start()
            hop(1, 1, 1)

        @pl.when(i == 4)
        def _():
            hop(1, 2, 0)

        @pl.when(i == 6)
        def _():
            hop(1, 2, 1)

        @pl.when(i == 3)
        def _():
            ss[3].wait_recv()
            vb[2] = vb[1] + vr[3]
            ss[4].start()
            dw_copy.wait_recv()
            for c in g3 + a3:
                c.wait_recv()

        for r_out in range(4):
            @pl.when(i == 4 + r_out)
            def _():
                dwa[0, rows(r_out), :] += dwr[rows(r_out), :]
                outs[r_out].start()
        return carry

    lax.fori_loop(0, 8, dw_step, 0)
    ss[4].wait_recv()
    loss_o[...] = vb[2] + vr[4]
    for c in rr[1][2]:
        c.wait_recv()
    dh_o[1] = dh[1, 0] + rs[1, 2]
    for c in outs:
        c.wait()
    for c in every:
        c.wait_send()


def solution(mesh):
    group = mesh.shape['fsdp']

    def local_head(hidden, targets, w_loc):
        valid = w_loc.shape[0]
        tokens = hidden.shape[1] * group
        bf = jnp.bfloat16
        any_spec = pl.BlockSpec(memory_space=pl.ANY)
        vmem = pl.BlockSpec(memory_space=pltpu.VMEM)
        loss, d_h, d_w = pl.pallas_call(
            functools.partial(head_kernel, group, valid, tokens),
            out_shape=[jax.ShapeDtypeStruct((16, LANES), F32), jax.ShapeDtypeStruct((2, TILE, 512), F32),
                       jax.ShapeDtypeStruct((valid, 512), F32)],
            in_specs=[any_spec, any_spec, vmem],
            out_specs=[vmem, vmem, any_spec],
            scratch_shapes=[
                pltpu.VMEM((3, 2, NZ, TILE, 512), bf),
                pltpu.VMEM((4, 2048, 512), bf),
                pltpu.VMEM((NZ, 8, TILE), F32),
                pltpu.VMEM((2, 8, TILE), F32),
                pltpu.VMEM((2, 3, 8, TILE), F32),
                pltpu.VMEM((3, 2, 8, TILE), F32),
                pltpu.VMEM((2, 3, TILE, 512), F32),
                pltpu.VMEM((2, NZ, TILE, 512), F32),
                pltpu.VMEM((2, 2048, 512), F32),
                pltpu.VMEM((2048, 512), F32),
                pltpu.VMEM((2, NZ, TILE, LANES), F32),
                pltpu.VMEM((2, NZ, TILE, LANES), F32),
                pltpu.VMEM((2, TILE, TILE), F32),
                pltpu.VMEM((TILE, LANES), F32),
                pltpu.VMEM((TILE, LANES), F32),
                pltpu.VMEM((2, 8, LANES), F32),
                pltpu.VMEM((3, 16, LANES), F32),
                pltpu.VMEM((5, 16, LANES), F32),
                pltpu.SemaphoreType.DMA((N_SEM,)),
                pltpu.SemaphoreType.DMA((N_SEM,)),
                pltpu.SemaphoreType.DMA((7,)),
            ],
            compiler_params=pltpu.CompilerParams(collective_id=0, has_side_effects=True, vmem_limit_bytes=67043328),
        )(hidden, w_loc, targets)
        loss_vals = jnp.sum(loss.reshape(2, 8 * LANES), axis=1) / tokens
        return loss_vals, d_h, d_w

    return jax.shard_map(local_head, mesh=mesh,
                         in_specs=(P(None, ('dp', 'fsdp'), None), P(None, ('dp', 'fsdp')), P('fsdp', None)),
                         out_specs=(P('dp'), P(None, ('dp', 'fsdp'), None), P(('dp', 'fsdp'), None)),
                         check_vma=False)
```
